32 devices in a mesh: rows: 32 (over z, y, x, core).
Axes of the slice: x: 2, y: 2, z: 4, core: 2. Of those that a mesh axis runs over, the one named last changes fastest.
Arguments:
- right_sides: float32 [32, 32768], P(None, 'rows'), may hold values from -48 to 48
- initial: float32 [32, 32768], P(None, 'rows'), may hold values from -1.2 to 1.2
- diag_blocks: float32 [32768, 256], P('rows'), may hold values from -2 to 9
- sub_blocks: float32 [32768, 256], P('rows'), may hold values from -0.21875 to 0.21875
- super_blocks: float32 [32768, 256], P('rows'), may hold values from -0.21875 to 0.21875
- local_inverse: bfloat16 [32768, 1024], P('rows'), may hold values from -1 to 1
- upper_spikes: bfloat16 [256, 32768], P(None, 'rows'), may hold values from -0.21875 to 0.21875
- lower_spikes: bfloat16 [256, 32768], P(None, 'rows'), may hold values from -2 to 2
Outputs:
- solution: float32 [32, 32768], P(None, 'rows')
- residual_norms: float32 [3, 32], replicated
The draws below stay inside these ranges and needn't reach their ends.
All inputs are finite; a program needn't handle non-finite values.
Results may differ from the reference program's by a relative error of at most 0.002.
The reference program's roundings to bfloat16 on the way (of `rounded`) count: a program that leaves them out, or rounds other values in their place, can miss the bound.
Values may be sent and summed in bfloat16 or wider, within the bound.
A program may use at most 64 MiB of HBM per device.

```python
import math
import jax
import jax.numpy as jnp
from jax import lax

BAND = 256
RHS = 32
ROWS_DEV = 1024
ITERS = 2
ORDER = 32768
N_ROWS = 32


def block_parts(key):
    base_key = jax.random.fold_in(key, 101)
    block_total = ORDER // BAND
    log_scales = jax.random.uniform(jax.random.fold_in(base_key, 1), (block_total, BAND), jnp.float32, math.log(2.0), math.log(8.0))
    mixing = jnp.clip(jax.random.normal(jax.random.fold_in(base_key, 2), (block_total, BAND, BAND), jnp.float32), -5.0, 5.0)
    return (jnp.exp(log_scales), mixing * (0.3 / math.sqrt(BAND)))


def draw_diag_blocks(key, part):
    scales, mixing = block_parts(key)
    unit_matrix = jnp.eye(BAND, dtype=jnp.float32)
    blocks = mixing + scales[:, :, None] * unit_matrix[None]
    return blocks.reshape(ORDER, BAND)


def draw_local_inverse(key, part):
    scales, mixing = block_parts(key)
    inverse_scale = 1.0 / scales
    unit_matrix = jnp.eye(BAND, dtype=jnp.float32)
    approx = inverse_scale[:, :, None] * unit_matrix[None] - inverse_scale[:, :, None] * mixing * inverse_scale[:, None, :]
    per_device = ROWS_DEV // BAND
    approx = approx.reshape(N_ROWS, per_device, BAND, BAND)
    positioned_rows = jnp.einsum('pkij,kl->pkilj', approx, jnp.eye(per_device, dtype=jnp.float32))
    noise = jnp.clip(jax.random.normal(jax.random.fold_in(key, 102), (N_ROWS, ROWS_DEV, ROWS_DEV), jnp.float32), -5.0, 5.0)
    whole = positioned_rows.reshape(N_ROWS, ROWS_DEV, ROWS_DEV) + noise * (0.06 / math.sqrt(ROWS_DEV))
    return jnp.clip(whole.reshape(ORDER, ROWS_DEV), -1.0, 1.0).astype(jnp.bfloat16)


def draw_lower_spikes(key, part):
    inner = jnp.clip(jax.random.normal(jax.random.fold_in(key, 21), (BAND, N_ROWS, ROWS_DEV - BAND), jnp.float32), -5.0, 5.0)
    inner = inner * (0.3 / math.sqrt(BAND))
    slow_share = 0.5
    slowness = jax.random.uniform(jax.random.fold_in(key, 22), (BAND,), jnp.float32) < slow_share
    fast_rate = jnp.exp(jax.random.uniform(jax.random.fold_in(key, 23), (BAND,), jnp.float32, math.log(0.15), math.log(1.0)))
    rates = jnp.where(slowness, 2.5 / N_ROWS, fast_rate)
    spread = jax.random.uniform(jax.random.fold_in(key, 24), (N_ROWS, BAND), jnp.float32, 0.6, 1.4)
    retain = jnp.exp(-rates[None, :] * spread)
    spike_position = jax.random.randint(jax.random.fold_in(key, 25), (3,), 0, N_ROWS)
    eliminated_rows = jnp.any(jnp.arange(N_ROWS)[:, None] == spike_position[None, :], axis=1)
    retain = jnp.where(eliminated_rows[:, None] & slowness[None, :], retain * 0.6, retain)
    mixing = jnp.clip(jax.random.normal(jax.random.fold_in(key, 26), (N_ROWS, BAND, BAND), jnp.float32), -5.0, 5.0)
    coupling = jnp.eye(BAND, dtype=jnp.float32)[None] + mixing * (0.2 / math.sqrt(BAND))
    tip_blocks = -(coupling * retain[:, None, :])
    tip_layout = jnp.transpose(tip_blocks, (1, 0, 2))
    whole = jnp.concatenate([inner, tip_layout], axis=2)
    return jnp.clip(whole.reshape(BAND, ORDER), -2.0, 2.0).astype(jnp.bfloat16)


def draw_right_sides(key, part):
    column = jnp.arange(ORDER, dtype=jnp.float32) / ORDER
    jitter = jax.random.uniform(jax.random.fold_in(key, 31), (ORDER,), jnp.float32, -1.15, 1.15)
    rough = jnp.clip(jax.random.normal(jax.random.fold_in(key, 34), (RHS, ORDER), jnp.float32), -4.0, 4.0)
    column_scale = jnp.exp(math.log(3.0) * column + jitter)
    values = rough * column_scale[None, :]
    return jnp.clip(values, -48.0, 48.0)


def block_levels(stream_key, dims, split, smallest, largest):
    gain = 1.0
    for axis_at, shards_of in split:
        steps = jax.random.uniform(jax.random.fold_in(jax.random.fold_in(stream_key, 6), axis_at), (shards_of,), jnp.float32, smallest / len(split), largest / len(split))
        gain = gain * jnp.repeat(jnp.exp(steps), dims[axis_at] // shards_of).reshape((-1,) + (1,) * (len(dims) - 1 - axis_at))
    return gain


def gaussian(stream_key, extent, width, reach, cuts=(), held_as=jnp.bfloat16):
    loudness = block_levels(stream_key, extent, cuts, -0.22, 0.18) if cuts else 1.0
    entries = jax.random.normal(stream_key, extent, jnp.float32) * width * loudness
    return jnp.minimum(jnp.maximum(entries, -reach), reach).astype(held_as)


def setup_inputs(seed: int = 0) -> dict:
    splits = jax.random.split(jax.random.key(seed), 9)
    return {
        "right_sides": draw_right_sides(jax.random.fold_in(splits[8], 71), 0),
        "initial": gaussian(splits[1], (RHS, ORDER), 0.2, 1.2, ((1, 32),), jnp.float32),
        "diag_blocks": draw_diag_blocks(jax.random.fold_in(splits[8], 71), 0),
        "sub_blocks": gaussian(splits[3], (ORDER, BAND), (3 * BAND) ** -0.5, 0.21875, ((0, 32),), jnp.float32),
        "super_blocks": gaussian(splits[4], (ORDER, BAND), (3 * BAND) ** -0.5, 0.21875, ((0, 32),), jnp.float32),
        "local_inverse": draw_local_inverse(jax.random.fold_in(splits[8], 71), 0),
        "upper_spikes": gaussian(splits[6], (BAND, ORDER), (3 * BAND) ** -0.5, 0.21875, ((1, 32),)),
        "lower_spikes": draw_lower_spikes(jax.random.fold_in(splits[8], 71), 0),
    }


maximum_level = lax.Precision.HIGHEST

def residual_of(right_sides, solution, diag_mat, lower_mat, upper_mat):
    padded = jnp.pad(solution, ((0, 0), (BAND, BAND)))
    stacked = padded.reshape(padded.shape[0], -1, BAND)
    applied = jnp.einsum('rkb,kbc->rkc', stacked[:, 1:-1], diag_mat, precision=maximum_level)
    applied = applied + jnp.einsum('rkb,kbc->rkc', stacked[:, :-2], lower_mat, precision=maximum_level)
    applied = applied + jnp.einsum('rkb,kbc->rkc', stacked[:, 2:], upper_mat, precision=maximum_level)
    return right_sides - applied.reshape(right_sides.shape)

def norm_row(residual):
    return jnp.sqrt(lax.optimization_barrier(jnp.sum(residual * residual, axis=1)) / ORDER)

def solve_partition(operands):
    return jnp.dot(operands[0].astype(jnp.float32), operands[1].astype(jnp.float32), precision=maximum_level)

def advance(carried, operands):
    current = operands[0] + jnp.dot(carried, operands[1], precision=maximum_level)
    return (current, (carried, current))

def rounded_copy(values):
    return lax.optimization_barrier(values.astype(jnp.bfloat16)).astype(jnp.float32)

def reference(right_sides, initial, diag_blocks, sub_blocks, super_blocks, local_inverse, upper_spikes, lower_spikes):
    diag_mat = diag_blocks.reshape(-1, BAND, BAND)
    lower_mat = sub_blocks.reshape(-1, BAND, BAND)
    upper_mat = super_blocks.reshape(-1, BAND, BAND)
    inverse_parts = local_inverse.reshape(N_ROWS, ROWS_DEV, ROWS_DEV)
    upper_pieces = upper_spikes.reshape(BAND, N_ROWS, ROWS_DEV).astype(jnp.float32)
    lower_pieces = lower_spikes.reshape(BAND, N_ROWS, ROWS_DEV).astype(jnp.float32)
    chain_mats = -jnp.transpose(lower_pieces[:, :, ROWS_DEV - BAND:], (1, 0, 2))
    bottom_upper = jnp.transpose(upper_pieces[:, :, ROWS_DEV - BAND:], (1, 0, 2))
    top_lower = jnp.transpose(lower_pieces[:, :, :BAND], (1, 0, 2))
    next_lower = jnp.concatenate([top_lower[1:], jnp.zeros_like(top_lower[:1])], axis=0)
    solution = initial
    records = []
    for turn_index in range(ITERS):
        residual = residual_of(right_sides, solution, diag_mat, lower_mat, upper_mat)
        records.append(norm_row(residual))
        rounded = residual.astype(jnp.bfloat16).reshape(RHS, N_ROWS, ROWS_DEV).transpose(1, 0, 2)
        local_part = lax.map(solve_partition, (rounded, inverse_parts))
        own_top = local_part[:, :, :BAND]
        next_top = jnp.concatenate([own_top[1:], jnp.zeros_like(own_top[:1])], axis=0)
        offset = local_part[:, :, ROWS_DEV - BAND:] - jnp.einsum('pri,pij->prj', next_top, bottom_upper, precision=maximum_level)
        leftover, outputs = lax.scan(advance, jnp.zeros((RHS, BAND), jnp.float32), (offset, chain_mats))
        previous, current = outputs
        top_tip = next_top - jnp.einsum('pri,pij->prj', current, next_lower, precision=maximum_level)
        correction = local_part - jnp.einsum('pri,ipm->prm', rounded_copy(top_tip), upper_pieces, precision=maximum_level)
        correction = correction - jnp.einsum('pri,ipm->prm', rounded_copy(previous), lower_pieces, precision=maximum_level)
        solution = solution + correction.transpose(1, 0, 2).reshape(RHS, ORDER)
    residual = residual_of(right_sides, solution, diag_mat, lower_mat, upper_mat)
    records.append(norm_row(residual))
    return (solution, jnp.stack(records))
```

```python
import jax
import jax.numpy as jnp
from jax import lax
from jax.experimental import pallas as pl
from jax.experimental.pallas import tpu as pltpu
from jax.sharding import PartitionSpec as P

ITERS = 2
GROUP = 8
SUB = 8
LANES = 128
F32 = jnp.float32
BF16 = jnp.bfloat16
MESH = pl.DeviceIdType.MESH


def rcopy(src, dst, send_sem, recv_sem, target):
    return pltpu.make_async_remote_copy(
        src_ref=src,
        dst_ref=dst,
        send_sem=send_sem,
        recv_sem=recv_sem,
        device_id=(target,),
        device_id_type=MESH,
    )


def stacked_split(v):
    hi = v.astype(BF16).astype(F32)
    return jnp.concatenate([hi, v - hi], axis=0).astype(BF16)


def dot(a, b):
    return jnp.dot(a, b, preferred_element_type=F32)


def fold(o):
    half = o.shape[0] // 2
    return o[:half] + o[half:]


def mm2(v, w):
    return fold(dot(stacked_split(v), w))


def make_kernel(n, rhs, cols, band):
    blocks = cols // band
    groups = n // GROUP
    rowblocks = rhs // SUB
    order = float(cols * n)
    tail = cols - band

    def kernel(
        b_hbm, x_hbm, d_hbm, lo_hbm, up_hbm, z_hbm, us_hbm, ls_hbm,
        out_ref, norm_ref,
        b, x, a_f32, z, us, ls, a_hi, a_lo, lg, w_hi, w_lo, uprev, lnext,
        halo_l, halo_r, loc, ntop, msg, inbuf, plbuf, bin_, bout, pout, prevbuf,
        nstack, nrow, nbuf,
        in_sem, l_send, l_recv, nb_send, nb_recv, halo_send, halo_recv,
        nt_send, nt_recv, a_send, a_recv, b_send, b_recv, p_send, p_recv,
        n_send, n_recv,
    ):
        me = lax.axis_index("rows")
        j = lax.rem(me, GROUP)
        g = me // GROUP
        base = me - j
        d = lax.rem(j, rowblocks)
        h = j // rowblocks
        partner = base + j + 1 - 2 * lax.rem(j, 2)
        left = lax.max(me - 1, 0)
        right = lax.min(me + 1, n - 1)
        has_left = me > 0
        has_right = me < n - 1

        loads = [
            pltpu.make_async_copy(x_hbm, x, in_sem.at[0]),
            pltpu.make_async_copy(ls_hbm.at[:, pl.ds(tail, band)], lg.at[j], in_sem.at[1]),
            pltpu.make_async_copy(us_hbm, us, in_sem.at[2]),
            pltpu.make_async_copy(ls_hbm, ls, in_sem.at[3]),
            pltpu.make_async_copy(d_hbm, a_f32.at[1], in_sem.at[4]),
            pltpu.make_async_copy(lo_hbm, a_f32.at[0], in_sem.at[5]),
            pltpu.make_async_copy(up_hbm, a_f32.at[2], in_sem.at[6]),
            pltpu.make_async_copy(b_hbm, b, in_sem.at[7]),
            pltpu.make_async_copy(z_hbm, z, in_sem.at[8]),
        ]
        for c in loads:
            c.start()

        barrier = pltpu.get_barrier_semaphore()

        @pl.loop(1, n)
        def _(k):
            pl.semaphore_signal(
                barrier, inc=1, device_id=(lax.rem(me + k, n),), device_id_type=MESH
            )

        @pl.when(me == 0)
        def _():
            halo_l[...] = jnp.zeros_like(halo_l)
            uprev[...] = jnp.zeros_like(uprev)

        @pl.when(me == n - 1)
        def _():
            halo_r[...] = jnp.zeros_like(halo_r)
            lnext[...] = jnp.zeros_like(lnext)
            ntop[...] = jnp.zeros_like(ntop)

        @pl.when(g == 0)
        def _():
            bin_[...] = jnp.zeros_like(bin_)

        nstack[...] = jnp.zeros_like(nstack)

        def halo_copies(it):
            to_right = rcopy(x.at[:, pl.ds(tail, band)], halo_l.at[it],
                             halo_send.at[it, 0], halo_recv.at[it, 0], right)
            to_left = rcopy(x.at[:, pl.ds(0, band)], halo_r.at[it],
                            halo_send.at[it, 1], halo_recv.at[it, 1], left)
            return to_right, to_left

        def halo_start(it):
            to_right, to_left = halo_copies(it)
            pl.when(has_right)(to_right.start)
            pl.when(has_left)(to_left.start)

        def halo_wait_recv(it):
            to_right, to_left = halo_copies(it)
            pl.when(has_left)(to_right.wait_recv)
            pl.when(has_right)(to_left.wait_recv)

        def halo_wait_send(it):
            to_right, to_left = halo_copies(it)
            pl.when(has_right)(to_right.wait_send)
            pl.when(has_left)(to_left.wait_send)

        loads[0].wait()
        loads[1].wait()
        pl.semaphore_wait(barrier, n - 1)
        halo_start(0)

        l_copies = [rcopy(lg.at[j], lg.at[j], l_send.at[0], l_recv.at[j], partner)]
        for k in range(1, GROUP // 2):
            l_copies.append(
                rcopy(lg.at[j], lg.at[j], l_send.at[k], l_recv.at[j],
                      base + lax.rem(j + 2 * k, GROUP))
            )
        for c in l_copies:
            c.start()
        loads[2].wait()
        loads[3].wait()
        u_copy = rcopy(us.at[:, pl.ds(tail, band)], uprev, nb_send.at[0], nb_recv.at[0], right)
        t_copy = rcopy(ls.at[:, pl.ds(0, band)], lnext, nb_send.at[1], nb_recv.at[1], left)
        pl.when(has_right)(u_copy.start)
        pl.when(has_left)(t_copy.start)

        for part, load in ((1, 4), (0, 5), (2, 6)):
            loads[load].wait()

            @pl.loop(0, blocks)
            def _(k):
                rows = pl.ds(pl.multiple_of(k * band, band), band)
                v = a_f32[part, rows, :]
                hi = v.astype(BF16)
                a_hi[part, k] = hi
                a_lo[part, k] = (v - hi.astype(F32)).astype(BF16)

        loads[7].wait()
        loads[8].wait()

        def residual(it):
            sp = [stacked_split(x[:, k * band:(k + 1) * band]) for k in range(blocks)]

            def term(s, part, k):
                return fold(dot(s, a_hi[part, k])) + dot(s[:rhs], a_lo[part, k])

            acc = []
            for k in range(blocks):
                t = b[:, k * band:(k + 1) * band] - term(sp[k], 1, k)
                if k > 0:
                    t = t - term(sp[k - 1], 0, k)
                if k < blocks - 1:
                    t = t - term(sp[k + 1], 2, k)
                acc.append(t)
            halo_wait_recv(it)
            acc[0] = acc[0] - term(stacked_split(halo_l[it]), 0, 0)
            acc[-1] = acc[-1] - term(stacked_split(halo_r[it]), 2, blocks - 1)
            sq = None
            for t in acc:
                for c in range(band // LANES):
                    v = t[:, c * LANES:(c + 1) * LANES]
                    sq = v * v if sq is None else sq + v * v
            nstack[it * rhs:(it + 1) * rhs, :] = sq
            return acc

        for it in range(ITERS):
            acc = residual(it)
            rounded = jnp.concatenate([t.astype(BF16) for t in acc], axis=1)
            top_own = dot(rounded, z[:, 0:band])
            loc[:, 0:band] = top_own
            nt_copy = rcopy(loc.at[:, pl.ds(0, band)], ntop.at[it],
                            nt_send.at[it], nt_recv.at[it], left)
            pl.when(has_left)(nt_copy.start)
            bot_own = dot(rounded, z[:, tail:])
            if it == 0:
                pl.when(has_left)(u_copy.wait_recv)
            tu = mm2(top_own, uprev[...])
            for r in range(rowblocks):
                msg[it, r, 0] = bot_own[r * SUB:(r + 1) * SUB]
                msg[it, r, 1] = tu[r * SUB:(r + 1) * SUB]
            a_copies = []
            for k in range(1, GROUP):
                t = lax.rem(j + k, GROUP)
                c = rcopy(msg.at[it, lax.rem(t, rowblocks)], inbuf.at[it, j],
                          a_send.at[it, k], a_recv.at[it, j], base + t)
                c.start()
                a_copies.append(c)
            inbuf[it, j] = msg[it, d]
            loc[:, tail:] = bot_own
            for k in range(1, blocks - 1):
                loc[:, k * band:(k + 1) * band] = dot(rounded, z[:, k * band:(k + 1) * band])

            if it == 0:
                for k in range(1, GROUP // 2):
                    owner = lax.rem(j + 2 * k, GROUP)
                    c = rcopy(lg.at[owner], lg.at[owner], l_send.at[GROUP // 2 - 1 + k],
                              l_recv.at[owner], partner)
                    c.wait_recv()
                    c.start()
                    l_copies.append(c)
                for k in range(GROUP // 2):
                    owner = lax.rem(j + 1 - 2 * lax.rem(j, 2) + 2 * k + GROUP, GROUP)
                    rcopy(lg.at[owner], lg.at[owner], l_send.at[0],
                          l_recv.at[owner], partner).wait_recv()
            for k in range(1, GROUP):
                t = lax.rem(j + k, GROUP)
                rcopy(msg.at[it, 0], inbuf.at[it, t], a_send.at[it, k],
                      a_recv.at[it, t], base + t).wait_recv()

            carry = jnp.where(g > 0, -inbuf[it, 0, 1], 0.0)
            plbuf[it, 0] = carry
            for q in range(GROUP):
                carry = inbuf[it, q, 0] - mm2(carry, lg[q])
                if q < GROUP - 1:
                    carry = carry - inbuf[it, q + 1, 1]
                    plbuf[it, q + 1] = carry
            group_end = carry

            bout[it] = group_end
            b_copy = rcopy(bout.at[it], bin_.at[it], b_send.at[it], b_recv.at[it],
                           lax.rem(me + GROUP, n))
            if groups > 1:
                pl.when(g == 0)(b_copy.start)

            if it == 0:
                row = lax.broadcasted_iota(jnp.int32, (band, band), 0)
                col = lax.broadcasted_iota(jnp.int32, (band, band), 1)
                w_hi[0] = jnp.where(row == col, 1.0, 0.0).astype(BF16)
                w_lo[0] = jnp.zeros((band, band), BF16)

                @pl.loop(0, GROUP)
                def _(q):
                    v = -(dot(w_hi[q], lg[q]) + dot(w_lo[q], lg[q]))
                    hi = v.astype(BF16)
                    w_hi[q + 1] = hi
                    w_lo[q + 1] = (v - hi.astype(F32)).astype(BF16)

            if groups > 1:

                @pl.when(g > 0)
                def _():
                    b_copy.wait_recv()

                    @pl.when(g < groups - 1)
                    def _():
                        s = stacked_split(bin_[it])
                        bout[it] = bout[it] + fold(dot(s, w_hi[GROUP])) + fold(dot(s, w_lo[GROUP]))
                        b_copy.start()

            s = stacked_split(bin_[it])
            for i in range(rowblocks):
                q = h * rowblocks + i
                pout[it, i] = plbuf[it, q] + fold(dot(s, w_hi[q])) + fold(dot(s, w_lo[q]))
            p_copies = []
            for k in range(1, rowblocks):
                i = lax.rem(d + k, rowblocks)
                c = rcopy(pout.at[it, i], prevbuf.at[it, d], p_send.at[it, k],
                          p_recv.at[it, d], base + h * rowblocks + i)
                c.start()
                p_copies.append(c)
            prevbuf[it, d] = pout[it, d]

            pl.when(has_right)(nt_copy.wait_recv)
            if it == 0:
                pl.when(has_right)(t_copy.wait_recv)
            next_top = ntop[it]
            offset = loc[:, tail:] - mm2(next_top, us[:, tail:])
            for k in range(1, rowblocks):
                i = lax.rem(d + k, rowblocks)
                rcopy(pout.at[it, i], prevbuf.at[it, i], p_send.at[it, k],
                      p_recv.at[it, i], base + h * rowblocks + i).wait_recv()
            previous = prevbuf[it].reshape(rhs, band)
            bottom = offset - mm2(previous, ls[:, tail:])
            top = next_top - mm2(bottom, lnext[...])
            top = jnp.where(has_right, top, 0.0).astype(BF16)
            prev16 = previous.astype(BF16)
            halo_wait_send(it)

            def update(k):
                c = slice(k * band, (k + 1) * band)
                x[:, c] = x[:, c] + (loc[:, c] - dot(top, us[:, c]) - dot(prev16, ls[:, c]))

            update(0)
            update(blocks - 1)
            halo_start(it + 1)
            for k in range(1, blocks - 1):
                update(k)
            pl.when(has_left)(nt_copy.wait_send)
            for c in a_copies:
                c.wait_send()
            for c in p_copies:
                c.wait_send()
            if groups > 1:
                pl.when(g < groups - 1)(b_copy.wait_send)
            if it == 0:
                for c in l_copies:
                    c.wait_send()
                pl.when(has_right)(u_copy.wait_send)
                pl.when(has_left)(t_copy.wait_send)

        out_ref[...] = x[...]
        residual(ITERS)
        partial = jnp.sum(nstack[...].T, axis=0, keepdims=True)
        nrow[...] = partial
        nbuf[me] = partial

        def norm_copy(k):
            return rcopy(nrow, nbuf.at[me], n_send.at[k], n_recv.at[me], lax.rem(me + k, n))

        @pl.loop(1, n)
        def _(k):
            norm_copy(k).start()

        halo_wait_send(ITERS)

        @pl.loop(1, n)
        def _(k):
            t = lax.rem(me + k, n)
            rcopy(nrow, nbuf.at[t], n_send.at[k], n_recv.at[t], t).wait_recv()

        total = jnp.sqrt(jnp.sum(nbuf[...], axis=0) / order)
        for i in range(ITERS + 1):
            norm_ref[i:i + 1, :] = total[:, i * rhs:(i + 1) * rhs]

        @pl.loop(1, n)
        def _(k):
            norm_copy(k).wait_send()

    return kernel


def body(b, x, dg, lo, up, z, us, ls):
    n = lax.axis_size("rows")
    rhs, cols = b.shape
    band = dg.shape[1]
    blocks = cols // band
    rb = rhs // SUB
    dma = pltpu.SemaphoreType.DMA
    vm = pltpu.VMEM
    scratch = [
        vm((rhs, cols), F32), vm((rhs, cols), F32), vm((3, cols, band), F32),
        vm(z.shape, BF16), vm(us.shape, BF16), vm(ls.shape, BF16),
        vm((3, blocks, band, band), BF16), vm((3, blocks, band, band), BF16),
        vm((GROUP, band, band), BF16),
        vm((GROUP + 1, band, band), BF16), vm((GROUP + 1, band, band), BF16),
        vm((band, band), BF16), vm((band, band), BF16),
        vm((ITERS + 1, rhs, band), F32), vm((ITERS + 1, rhs, band), F32),
        vm((rhs, cols), F32), vm((ITERS, rhs, band), F32),
        vm((ITERS, rb, 2, SUB, band), F32), vm((ITERS, GROUP, 2, SUB, band), F32),
        vm((ITERS, GROUP, SUB, band), F32),
        vm((ITERS, SUB, band), F32), vm((ITERS, SUB, band), F32),
        vm((ITERS, rb, SUB, band), F32), vm((ITERS, rb, SUB, band), F32),
        vm((LANES, LANES), F32), vm((1, LANES), F32), vm((n, 1, LANES), F32),
        dma((9,)), dma((GROUP,)), dma((GROUP,)), dma((2,)), dma((2,)),
        dma((ITERS + 1, 2)), dma((ITERS + 1, 2)),
        dma((ITERS,)), dma((ITERS,)), dma((ITERS, GROUP)), dma((ITERS, GROUP)),
        dma((ITERS,)), dma((ITERS,)), dma((ITERS, rb)), dma((ITERS, rb)),
        dma((n,)), dma((n,)),
    ]
    return pl.pallas_call(
        make_kernel(n, rhs, cols, band),
        out_shape=(
            jax.ShapeDtypeStruct((rhs, cols), F32),
            jax.ShapeDtypeStruct((ITERS + 1, rhs), F32),
        ),
        in_specs=[pl.BlockSpec(memory_space=pl.ANY)] * 8,
        out_specs=(pl.BlockSpec(memory_space=pltpu.VMEM),) * 2,
        scratch_shapes=scratch,
        compiler_params=pltpu.CompilerParams(
            collective_id=0, has_side_effects=True, vmem_limit_bytes=48 * 1024 * 1024
        ),
    )(b, x, dg, lo, up, z, us, ls)


def solution(mesh):
    return jax.shard_map(
        body,
        mesh=mesh,
        in_specs=(
            P(None, "rows"),
            P(None, "rows"),
            P("rows", None),
            P("rows", None),
            P("rows", None),
            P("rows", None),
            P(None, "rows"),
            P(None, "rows"),
        ),
        out_specs=(P(None, "rows"), P()),
        check_vma=False,
    )
```

```python
import jax
import jax.numpy as jnp
from jax import lax
from jax.experimental import pallas as pl
from jax.experimental.pallas import tpu as pltpu
from jax.sharding import PartitionSpec as P

ITERS = 2
GROUP = 8
SUB = 8
LANES = 128
F32 = jnp.float32
BF16 = jnp.bfloat16
MESH = pl.DeviceIdType.MESH


def rcopy(src, dst, send_sem, recv_sem, target):
    return pltpu.make_async_remote_copy(
        src_ref=src,
        dst_ref=dst,
        send_sem=send_sem,
        recv_sem=recv_sem,
        device_id=(target,),
        device_id_type=MESH,
    )


def stacked_split(v):
    hi = v.astype(BF16).astype(F32)
    return jnp.concatenate([hi, v - hi], axis=0).astype(BF16)


def dot(a, b):
    return jnp.dot(a, b, preferred_element_type=F32)


def fold(o):
    half = o.shape[0] // 2
    return o[:half] + o[half:]


def mm2(v, w):
    return fold(dot(stacked_split(v), w))


def make_kernel(n, rhs, cols, band):
    blocks = cols // band
    groups = n // GROUP
    rowblocks = rhs // SUB
    order = float(cols * n)
    tail = cols - band

    def kernel(
        b_hbm, x_hbm, d_hbm, lo_hbm, up_hbm, z_hbm, us_hbm, ls_hbm,
        out_ref, norm_ref,
        b, x, a_f32, z, us, ls, a_hi, a_lo, lg, w_hi, w_lo, uprev, lnext,
        halo_l, halo_r, loc, ntop, msg, inbuf, plbuf, bin_, bout, pout, prevbuf,
        nstack, nrow, nbuf,
        in_sem, l_send, l_recv, nb_send, nb_recv, halo_send, halo_recv,
        nt_send, nt_recv, a_send, a_recv, b_send, b_recv, p_send, p_recv,
        n_send, n_recv,
    ):
        me = lax.axis_index("rows")
        j = lax.rem(me, GROUP)
        g = me // GROUP
        base = me - j
        d = lax.rem(j, rowblocks)
        h = j // rowblocks
        partner = base + j + 1 - 2 * lax.rem(j, 2)
        left = lax.max(me - 1, 0)
        right = lax.min(me + 1, n - 1)
        has_left = me > 0
        has_right = me < n - 1

        loads = [
            pltpu.make_async_copy(x_hbm, x, in_sem.at[0]),
            pltpu.make_async_copy(ls_hbm.at[:, pl.ds(tail, band)], lg.at[j], in_sem.at[1]),
            pltpu.make_async_copy(us_hbm, us, in_sem.at[2]),
            pltpu.make_async_copy(ls_hbm, ls, in_sem.at[3]),
            pltpu.make_async_copy(d_hbm, a_f32.at[1], in_sem.at[4]),
            pltpu.make_async_copy(lo_hbm, a_f32.at[0], in_sem.at[5]),
            pltpu.make_async_copy(up_hbm, a_f32.at[2], in_sem.at[6]),
            pltpu.make_async_copy(b_hbm, b, in_sem.at[7]),
            pltpu.make_async_copy(z_hbm, z, in_sem.at[8]),
        ]
        for c in loads:
            c.start()

        barrier = pltpu.get_barrier_semaphore()

        @pl.loop(1, n)
        def _(k):
            pl.semaphore_signal(
                barrier, inc=1, device_id=(lax.rem(me + k, n),), device_id_type=MESH
            )

        @pl.when(me == 0)
        def _():
            halo_l[...] = jnp.zeros_like(halo_l)
            uprev[...] = jnp.zeros_like(uprev)

        @pl.when(me == n - 1)
        def _():
            halo_r[...] = jnp.zeros_like(halo_r)
            lnext[...] = jnp.zeros_like(lnext)
            ntop[...] = jnp.zeros_like(ntop)

        @pl.when(g == 0)
        def _():
            bin_[...] = jnp.zeros_like(bin_)

        nstack[...] = jnp.zeros_like(nstack)

        def halo_copies(it):
            to_right = rcopy(x.at[:, pl.ds(tail, band)], halo_l.at[it],
                             halo_send.at[it, 0], halo_recv.at[it, 0], right)
            to_left = rcopy(x.at[:, pl.ds(0, band)], halo_r.at[it],
                            halo_send.at[it, 1], halo_recv.at[it, 1], left)
            return to_right, to_left

        def halo_start(it):
            to_right, to_left = halo_copies(it)
            pl.when(has_right)(to_right.start)
            pl.when(has_left)(to_left.start)

        def halo_wait_recv(it):
            to_right, to_left = halo_copies(it)
            pl.when(has_left)(to_right.wait_recv)
            pl.when(has_right)(to_left.wait_recv)

        def halo_wait_send(it):
            to_right, to_left = halo_copies(it)
            pl.when(has_right)(to_right.wait_send)
            pl.when(has_left)(to_left.wait_send)

        loads[0].wait()
        loads[1].wait()
        pl.semaphore_wait(barrier, n - 1)
        halo_start(0)

        l_copies = [rcopy(lg.at[j], lg.at[j], l_send.at[0], l_recv.at[j], partner)]
        for k in range(1, GROUP // 2):
            l_copies.append(
                rcopy(lg.at[j], lg.at[j], l_send.at[k], l_recv.at[j],
                      base + lax.rem(j + 2 * k, GROUP))
            )
        loads[2].wait()
        loads[3].wait()
        u_copy = rcopy(us.at[:, pl.ds(tail, band)], uprev, nb_send.at[0], nb_recv.at[0], right)
        t_copy = rcopy(ls.at[:, pl.ds(0, band)], lnext, nb_send.at[1], nb_recv.at[1], left)
        pl.when(has_right)(u_copy.start)
        for c in l_copies:
            c.start()

        for part, load in ((1, 4), (0, 5), (2, 6)):
            loads[load].wait()

            @pl.loop(0, blocks)
            def _(k):
                rows = pl.ds(pl.multiple_of(k * band, band), band)
                v = a_f32[part, rows, :]
                hi = v.astype(BF16)
                a_hi[part, k] = hi
                a_lo[part, k] = (v - hi.astype(F32)).astype(BF16)

        loads[7].wait()
        loads[8].wait()

        def residual(it):
            sp = [stacked_split(x[:, k * band:(k + 1) * band]) for k in range(blocks)]

            def term(s, part, k):
                return fold(dot(s, a_hi[part, k])) + dot(s[:rhs], a_lo[part, k])

            acc = []
            for k in range(blocks):
                t = b[:, k * band:(k + 1) * band] - term(sp[k], 1, k)
                if k > 0:
                    t = t - term(sp[k - 1], 0, k)
                if k < blocks - 1:
                    t = t - term(sp[k + 1], 2, k)
                acc.append(t)
            halo_wait_recv(it)
            acc[0] = acc[0] - term(stacked_split(halo_l[it]), 0, 0)
            acc[-1] = acc[-1] - term(stacked_split(halo_r[it]), 2, blocks - 1)
            sq = None
            for t in acc:
                for c in range(band // LANES):
                    v = t[:, c * LANES:(c + 1) * LANES]
                    sq = v * v if sq is None else sq + v * v
            nstack[it * rhs:(it + 1) * rhs, :] = sq
            return acc

        for it in range(ITERS):
            acc = residual(it)
            rounded = jnp.concatenate([t.astype(BF16) for t in acc], axis=1)
            top_own = dot(rounded, z[:, 0:band])
            loc[:, 0:band] = top_own
            nt_copy = rcopy(loc.at[:, pl.ds(0, band)], ntop.at[it],
                            nt_send.at[it], nt_recv.at[it], left)
            pl.when(has_left)(nt_copy.start)
            bot_own = dot(rounded, z[:, tail:])
            if it == 0:
                pl.when(has_left)(u_copy.wait_recv)
            tu = mm2(top_own, uprev[...])
            for r in range(rowblocks):
                msg[it, r, 0] = bot_own[r * SUB:(r + 1) * SUB]
                msg[it, r, 1] = tu[r * SUB:(r + 1) * SUB]
            a_copies = []
            for k in range(1, GROUP):
                t = lax.rem(j + k, GROUP)
                c = rcopy(msg.at[it, lax.rem(t, rowblocks)], inbuf.at[it, j],
                          a_send.at[it, k], a_recv.at[it, j], base + t)
                c.start()
                a_copies.append(c)
            inbuf[it, j] = msg[it, d]
            loc[:, tail:] = bot_own
            for k in range(1, blocks - 1):
                loc[:, k * band:(k + 1) * band] = dot(rounded, z[:, k * band:(k + 1) * band])

            if it == 0:
                for k in range(1, GROUP // 2):
                    owner = lax.rem(j + 2 * k, GROUP)
                    c = rcopy(lg.at[owner], lg.at[owner], l_send.at[GROUP // 2 - 1 + k],
                              l_recv.at[owner], partner)
                    c.wait_recv()
                    c.start()
                    l_copies.append(c)
                pl.when(has_left)(t_copy.start)
                for k in range(GROUP // 2):
                    owner = lax.rem(j + 1 - 2 * lax.rem(j, 2) + 2 * k + GROUP, GROUP)
                    rcopy(lg.at[owner], lg.at[owner], l_send.at[0],
                          l_recv.at[owner], partner).wait_recv()
            for k in range(1, GROUP):
                t = lax.rem(j + k, GROUP)
                rcopy(msg.at[it, 0], inbuf.at[it, t], a_send.at[it, k],
                      a_recv.at[it, t], base + t).wait_recv()

            carry = jnp.where(g > 0, -inbuf[it, 0, 1], 0.0)
            plbuf[it, 0] = carry
            for q in range(GROUP):
                carry = inbuf[it, q, 0] - mm2(carry, lg[q])
                if q < GROUP - 1:
                    carry = carry - inbuf[it, q + 1, 1]
                    plbuf[it, q + 1] = carry
            group_end = carry

            bout[it] = group_end
            b_copy = rcopy(bout.at[it], bin_.at[it], b_send.at[it], b_recv.at[it],
                           lax.rem(me + GROUP, n))
            if groups > 1:
                pl.when(g == 0)(b_copy.start)

            if it == 0:
                row = lax.broadcasted_iota(jnp.int32, (band, band), 0)
                col = lax.broadcasted_iota(jnp.int32, (band, band), 1)
                w_hi[0] = jnp.where(row == col, 1.0, 0.0).astype(BF16)
                w_lo[0] = jnp.zeros((band, band), BF16)
                w_hi[1] = -lg[0]
                w_lo[1] = jnp.zeros((band, band), BF16)

                @pl.loop(1, GROUP)
                def _(q):
                    v = -(dot(w_hi[q], lg[q]) + dot(w_lo[q], lg[q]))
                    hi = v.astype(BF16)
                    w_hi[q + 1] = hi
                    w_lo[q + 1] = (v - hi.astype(F32)).astype(BF16)

            if groups > 1:

                @pl.when(g > 0)
                def _():
                    b_copy.wait_recv()

                    @pl.when(g < groups - 1)
                    def _():
                        s = stacked_split(bin_[it])
                        bout[it] = bout[it] + fold(dot(s, w_hi[GROUP])) + fold(dot(s, w_lo[GROUP]))
                        b_copy.start()

            s = stacked_split(bin_[it])
            for i in range(rowblocks):
                q = h * rowblocks + i
                pout[it, i] = plbuf[it, q] + fold(dot(s, w_hi[q])) + fold(dot(s, w_lo[q]))
            p_copies = []
            for k in range(1, rowblocks):
                i = lax.rem(d + k, rowblocks)
                c = rcopy(pout.at[it, i], prevbuf.at[it, d], p_send.at[it, k],
                          p_recv.at[it, d], base + h * rowblocks + i)
                c.start()
                p_copies.append(c)
            prevbuf[it, d] = pout[it, d]

            pl.when(has_right)(nt_copy.wait_recv)
            if it == 0:
                pl.when(has_right)(t_copy.wait_recv)
            next_top = ntop[it]
            offset = loc[:, tail:] - mm2(next_top, us[:, tail:])
            for k in range(1, rowblocks):
                i = lax.rem(d + k, rowblocks)
                rcopy(pout.at[it, i], prevbuf.at[it, i], p_send.at[it, k],
                      p_recv.at[it, i], base + h * rowblocks + i).wait_recv()
            previous = prevbuf[it].reshape(rhs, band)
            bottom = offset - mm2(previous, ls[:, tail:])
            top = next_top - mm2(bottom, lnext[...])
            top = jnp.where(has_right, top, 0.0).astype(BF16)
            prev16 = previous.astype(BF16)
            halo_wait_send(it)

            def update(k):
                c = slice(k * band, (k + 1) * band)
                x[:, c] = x[:, c] + (loc[:, c] - dot(top, us[:, c]) - dot(prev16, ls[:, c]))

            update(0)
            update(blocks - 1)
            halo_start(it + 1)
            for k in range(1, blocks - 1):
                update(k)
            pl.when(has_left)(nt_copy.wait_send)
            for c in a_copies:
                c.wait_send()
            for c in p_copies:
                c.wait_send()
            if groups > 1:
                pl.when(g < groups - 1)(b_copy.wait_send)
            if it == 0:
                for c in l_copies:
                    c.wait_send()
                pl.when(has_right)(u_copy.wait_send)
                pl.when(has_left)(t_copy.wait_send)

        out_ref[...] = x[...]
        residual(ITERS)
        partial = jnp.sum(nstack[...].T, axis=0, keepdims=True)
        nrow[...] = partial
        nbuf[me] = partial

        def norm_copy(k):
            return rcopy(nrow, nbuf.at[me], n_send.at[0], n_recv.at[0], lax.rem(me + k, n))

        @pl.loop(0, (n - 1) // 2)
        def _(i):
            norm_copy(n // 2 + i).start()
            norm_copy(n // 2 - 1 - i).start()

        norm_copy(n - 1).start()
        halo_wait_send(ITERS)
        everyone = nbuf.at[pl.ds(0, n - 1)]
        everything = rcopy(everyone, everyone, n_send.at[0], n_recv.at[0], right)
        everything.wait_recv()
        total = jnp.sqrt(jnp.sum(nbuf[...], axis=0) / order)
        for i in range(ITERS + 1):
            norm_ref[i:i + 1, :] = total[:, i * rhs:(i + 1) * rhs]
        everything.wait_send()

    return kernel


def body(b, x, dg, lo, up, z, us, ls):
    n = lax.axis_size("rows")
    rhs, cols = b.shape
    band = dg.shape[1]
    blocks = cols // band
    rb = rhs // SUB
    dma = pltpu.SemaphoreType.DMA
    vm = pltpu.VMEM
    scratch = [
        vm((rhs, cols), F32), vm((rhs, cols), F32), vm((3, cols, band), F32),
        vm(z.shape, BF16), vm(us.shape, BF16), vm(ls.shape, BF16),
        vm((3, blocks, band, band), BF16), vm((3, blocks, band, band), BF16),
        vm((GROUP, band, band), BF16),
        vm((GROUP + 1, band, band), BF16), vm((GROUP + 1, band, band), BF16),
        vm((band, band), BF16), vm((band, band), BF16),
        vm((ITERS + 1, rhs, band), F32), vm((ITERS + 1, rhs, band), F32),
        vm((rhs, cols), F32), vm((ITERS, rhs, band), F32),
        vm((ITERS, rb, 2, SUB, band), F32), vm((ITERS, GROUP, 2, SUB, band), F32),
        vm((ITERS, GROUP, SUB, band), F32),
        vm((ITERS, SUB, band), F32), vm((ITERS, SUB, band), F32),
        vm((ITERS, rb, SUB, band), F32), vm((ITERS, rb, SUB, band), F32),
        vm((LANES, LANES), F32), vm((1, LANES), F32), vm((n, 1, LANES), F32),
        dma((9,)), dma((GROUP,)), dma((GROUP,)), dma((2,)), dma((2,)),
        dma((ITERS + 1, 2)), dma((ITERS + 1, 2)),
        dma((ITERS,)), dma((ITERS,)), dma((ITERS, GROUP)), dma((ITERS, GROUP)),
        dma((ITERS,)), dma((ITERS,)), dma((ITERS, rb)), dma((ITERS, rb)),
        dma((1,)), dma((1,)),
    ]
    return pl.pallas_call(
        make_kernel(n, rhs, cols, band),
        out_shape=(
            jax.ShapeDtypeStruct((rhs, cols), F32),
            jax.ShapeDtypeStruct((ITERS + 1, rhs), F32),
        ),
        in_specs=[pl.BlockSpec(memory_space=pl.ANY)] * 8,
        out_specs=(pl.BlockSpec(memory_space=pltpu.VMEM),) * 2,
        scratch_shapes=scratch,
        compiler_params=pltpu.CompilerParams(
            collective_id=0, has_side_effects=True, vmem_limit_bytes=67043328
        ),
    )(b, x, dg, lo, up, z, us, ls)


def solution(mesh):
    return jax.shard_map(
        body,
        mesh=mesh,
        in_specs=(
            P(None, "rows"),
            P(None, "rows"),
            P("rows", None),
            P("rows", None),
            P("rows", None),
            P("rows", None),
            P(None, "rows"),
            P(None, "rows"),
        ),
        out_specs=(P(None, "rows"), P()),
        check_vma=False,
    )
```

```python
import jax
import jax.numpy as jnp
from jax import lax
from jax.experimental import pallas as pl
from jax.experimental.pallas import tpu as pltpu
from jax.sharding import PartitionSpec as P

ITERS = 2
GROUP = 8
SUB = 8
LANES = 128
F32 = jnp.float32
BF16 = jnp.bfloat16
MESH = pl.DeviceIdType.MESH


def rcopy(src, dst, send_sem, recv_sem, target):
    return pltpu.make_async_remote_copy(
        src_ref=src,
        dst_ref=dst,
        send_sem=send_sem,
        recv_sem=recv_sem,
        device_id=(target,),
        device_id_type=MESH,
    )


def stacked_split(v):
    hi = v.astype(BF16).astype(F32)
    return jnp.concatenate([hi, v - hi], axis=0).astype(BF16)


def dot(a, b):
    return jnp.dot(a, b, preferred_element_type=F32)


def fold(o):
    half = o.shape[0] // 2
    return o[:half] + o[half:]


def mm2(v, w):
    return fold(dot(stacked_split(v), w))


def make_kernel(n, rhs, cols, band):
    blocks = cols // band
    groups = n // GROUP
    rowblocks = rhs // SUB
    order = float(cols * n)
    tail = cols - band

    def kernel(
        b_hbm, x_hbm, d_hbm, lo_hbm, up_hbm, z_hbm, us_hbm, ls_hbm,
        out_ref, norm_ref,
        b, x, a_f32, z, us, ls, a_hi, a_lo, lg, w_hi, w_lo, uprev, lnext,
        halo_l, halo_r, loc, ntop, msg, inbuf, plbuf, bin_, bout, pout, prevbuf,
        nstack, nrow, nbuf,
        in_sem, l_send, l_recv, nb_send, nb_recv, halo_send, halo_recv,
        nt_send, nt_recv, a_send, a_recv, b_send, b_recv, p_send, p_recv,
        n_send, n_recv,
    ):
        me = lax.axis_index("rows")
        j = lax.rem(me, GROUP)
        g = me // GROUP
        base = me - j
        d = lax.rem(j, rowblocks)
        h = j // rowblocks
        partner = base + j + 1 - 2 * lax.rem(j, 2)
        left = lax.max(me - 1, 0)
        right = lax.min(me + 1, n - 1)
        has_left = me > 0
        has_right = me < n - 1

        barrier = pltpu.get_barrier_semaphore()

        def greet(k):
            pl.semaphore_signal(
                barrier, inc=1, device_id=(lax.rem(me + k, n),), device_id_type=MESH
            )

        greet(n - 1)

        @pl.loop(0, (n - 1) // 2)
        def _(i):
            greet(1 + i)
            greet(n - 2 - i)

        loads = [
            pltpu.make_async_copy(x_hbm, x, in_sem.at[0]),
            pltpu.make_async_copy(ls_hbm.at[:, pl.ds(tail, band)], lg.at[j], in_sem.at[1]),
            pltpu.make_async_copy(us_hbm, us, in_sem.at[2]),
            pltpu.make_async_copy(ls_hbm, ls, in_sem.at[3]),
            pltpu.make_async_copy(d_hbm, a_f32.at[1], in_sem.at[4]),
            pltpu.make_async_copy(lo_hbm, a_f32.at[0], in_sem.at[5]),
            pltpu.make_async_copy(up_hbm, a_f32.at[2], in_sem.at[6]),
            pltpu.make_async_copy(b_hbm, b, in_sem.at[7]),
            pltpu.make_async_copy(z_hbm, z, in_sem.at[8]),
        ]
        for c in loads:
            c.start()

        @pl.when(me == 0)
        def _():
            halo_l[...] = jnp.zeros_like(halo_l)
            uprev[...] = jnp.zeros_like(uprev)

        @pl.when(me == n - 1)
        def _():
            halo_r[...] = jnp.zeros_like(halo_r)
            lnext[...] = jnp.zeros_like(lnext)
            ntop[...] = jnp.zeros_like(ntop)

        @pl.when(g == 0)
        def _():
            bin_[...] = jnp.zeros_like(bin_)

        nstack[...] = jnp.zeros_like(nstack)

        def halo_copies(it):
            to_right = rcopy(x.at[:, pl.ds(tail, band)], halo_l.at[it],
                             halo_send.at[it, 0], halo_recv.at[it, 0], right)
            to_left = rcopy(x.at[:, pl.ds(0, band)], halo_r.at[it],
                            halo_send.at[it, 1], halo_recv.at[it, 1], left)
            return to_right, to_left

        def halo_start(it):
            to_right, to_left = halo_copies(it)
            pl.when(has_right)(to_right.start)
            pl.when(has_left)(to_left.start)

        def halo_wait_recv(it):
            to_right, to_left = halo_copies(it)
            pl.when(has_left)(to_right.wait_recv)
            pl.when(has_right)(to_left.wait_recv)

        def halo_wait_send(it):
            to_right, to_left = halo_copies(it)
            pl.when(has_right)(to_right.wait_send)
            pl.when(has_left)(to_left.wait_send)

        loads[0].wait()
        loads[1].wait()
        pl.semaphore_wait(barrier, n - 1)
        halo_start(0)

        core = lax.rem(j, 2)
        xflip = j + 2 - 4 * lax.rem(j // 2, 2)
        yflip = j + 4 - 8 * lax.rem(j // 4, 2)
        both = xflip + yflip - j
        relay = (1 - core) * xflip + core * yflip
        onward = (1 - core) * yflip + core * xflip

        def l_copy(owner, slot, target):
            return rcopy(lg.at[owner], lg.at[owner], l_send.at[slot], l_recv.at[owner],
                         base + target)

        buddy = partner - base
        l_copies = [
            l_copy(j, 0, buddy),
            l_copy(j, 1, relay),
            l_copy(j, 2, onward),
        ]
        loads[2].wait()
        loads[3].wait()
        u_copy = rcopy(us.at[:, pl.ds(tail, band)], uprev, nb_send.at[0], nb_recv.at[0], right)
        t_copy = rcopy(ls.at[:, pl.ds(0, band)], lnext, nb_send.at[1], nb_recv.at[1], left)
        pl.when(has_right)(u_copy.start)
        for c in l_copies:
            c.start()

        for part, load in ((1, 4), (0, 5), (2, 6)):
            loads[load].wait()

            @pl.loop(0, blocks)
            def _(k):
                rows = pl.ds(pl.multiple_of(k * band, band), band)
                v = a_f32[part, rows, :]
                hi = v.astype(BF16)
                a_hi[part, k] = hi
                a_lo[part, k] = (v - hi.astype(F32)).astype(BF16)

        loads[7].wait()
        loads[8].wait()

        def forward(owner, slot, target):
            c = l_copy(owner, slot, target)
            c.wait_recv()
            c.start()
            l_copies.append(c)

        def residual(it):
            sp = [stacked_split(x[:, k * band:(k + 1) * band]) for k in range(blocks)]

            def term(s, part, k):
                return fold(dot(s, a_hi[part, k])) + dot(s[:rhs], a_lo[part, k])

            acc = []
            for k in range(blocks):
                t = b[:, k * band:(k + 1) * band] - term(sp[k], 1, k)
                if k > 0:
                    t = t - term(sp[k - 1], 0, k)
                if k < blocks - 1:
                    t = t - term(sp[k + 1], 2, k)
                acc.append(t)
            if it == 0:
                l_copy(relay, 0, buddy).wait_recv()
                for slot, target in ((6, onward), (3, buddy)):
                    c = l_copy(relay, slot, target)
                    c.start()
                    l_copies.append(c)
            halo_wait_recv(it)
            acc[0] = acc[0] - term(stacked_split(halo_l[it]), 0, 0)
            acc[-1] = acc[-1] - term(stacked_split(halo_r[it]), 2, blocks - 1)
            sq = None
            for t in acc:
                for c in range(band // LANES):
                    v = t[:, c * LANES:(c + 1) * LANES]
                    sq = v * v if sq is None else sq + v * v
            nstack[it * rhs:(it + 1) * rhs, :] = sq
            return acc

        for it in range(ITERS):
            acc = residual(it)
            rounded = jnp.concatenate([t.astype(BF16) for t in acc], axis=1)
            top_own = dot(rounded, z[:, 0:band])
            loc[:, 0:band] = top_own
            nt_copy = rcopy(loc.at[:, pl.ds(0, band)], ntop.at[it],
                            nt_send.at[it], nt_recv.at[it], left)
            pl.when(has_left)(nt_copy.start)
            bot_own = dot(rounded, z[:, tail:])
            if it == 0:
                pl.when(has_left)(u_copy.wait_recv)
            tu = mm2(top_own, uprev[...])
            for r in range(rowblocks):
                msg[it, r, 0] = bot_own[r * SUB:(r + 1) * SUB]
                msg[it, r, 1] = tu[r * SUB:(r + 1) * SUB]
            a_copies = []
            for k in range(1, GROUP):
                t = lax.rem(j + k, GROUP)
                c = rcopy(msg.at[it, lax.rem(t, rowblocks)], inbuf.at[it, j],
                          a_send.at[it, k], a_recv.at[it, j], base + t)
                c.start()
                a_copies.append(c)
            inbuf[it, j] = msg[it, d]
            loc[:, tail:] = bot_own
            for k in range(1, blocks - 1):
                loc[:, k * band:(k + 1) * band] = dot(rounded, z[:, k * band:(k + 1) * band])

            if it == 0:
                for slot, owner in ((4, onward), (5, both)):
                    forward(owner, slot, buddy)
                pl.when(has_left)(t_copy.start)
                for k in range(GROUP // 2):
                    owner = lax.rem(j + 1 - 2 * lax.rem(j, 2) + 2 * k + GROUP, GROUP)
                    rcopy(lg.at[owner], lg.at[owner], l_send.at[0],
                          l_recv.at[owner], partner).wait_recv()
            for k in range(1, GROUP):
                t = lax.rem(j + k, GROUP)
                rcopy(msg.at[it, 0], inbuf.at[it, t], a_send.at[it, k],
                      a_recv.at[it, t], base + t).wait_recv()

            carry = jnp.where(g > 0, -inbuf[it, 0, 1], 0.0)
            plbuf[it, 0] = carry
            for q in range(GROUP):
                carry = inbuf[it, q, 0] - mm2(carry, lg[q])
                if q < GROUP - 1:
                    carry = carry - inbuf[it, q + 1, 1]
                    plbuf[it, q + 1] = carry
            group_end = carry

            bout[it] = group_end
            b_copy = rcopy(bout.at[it], bin_.at[it], b_send.at[it], b_recv.at[it],
                           lax.rem(me + GROUP, n))
            if groups > 1:
                pl.when(g == 0)(b_copy.start)

            if it == 0:
                row = lax.broadcasted_iota(jnp.int32, (band, band), 0)
                col = lax.broadcasted_iota(jnp.int32, (band, band), 1)
                w_hi[0] = jnp.where(row == col, 1.0, 0.0).astype(BF16)
                w_lo[0] = jnp.zeros((band, band), BF16)
                w_hi[1] = -lg[0]
                w_lo[1] = jnp.zeros((band, band), BF16)

                @pl.loop(1, GROUP)
                def _(q):
                    v = -(dot(w_hi[q], lg[q]) + dot(w_lo[q], lg[q]))
                    hi = v.astype(BF16)
                    w_hi[q + 1] = hi
                    w_lo[q + 1] = (v - hi.astype(F32)).astype(BF16)

            if groups > 1:

                @pl.when(g > 0)
                def _():
                    b_copy.wait_recv()

                    @pl.when(g < groups - 1)
                    def _():
                        s = stacked_split(bin_[it])
                        bout[it] = bout[it] + fold(dot(s, w_hi[GROUP])) + fold(dot(s, w_lo[GROUP]))
                        b_copy.start()

            s = stacked_split(bin_[it])
            for i in range(rowblocks):
                q = h * rowblocks + i
                pout[it, i] = plbuf[it, q] + fold(dot(s, w_hi[q])) + fold(dot(s, w_lo[q]))
            p_copies = []
            for k in range(1, rowblocks):
                i = lax.rem(d + k, rowblocks)
                c = rcopy(pout.at[it, i], prevbuf.at[it, d], p_send.at[it, k],
                          p_recv.at[it, d], base + h * rowblocks + i)
                c.start()
                p_copies.append(c)
            prevbuf[it, d] = pout[it, d]

            pl.when(has_right)(nt_copy.wait_recv)
            if it == 0:
                pl.when(has_right)(t_copy.wait_recv)
            next_top = ntop[it]
            offset = loc[:, tail:] - mm2(next_top, us[:, tail:])
            for k in range(1, rowblocks):
                i = lax.rem(d + k, rowblocks)
                rcopy(pout.at[it, i], prevbuf.at[it, i], p_send.at[it, k],
                      p_recv.at[it, i], base + h * rowblocks + i).wait_recv()
            previous = prevbuf[it].reshape(rhs, band)
            bottom = offset - mm2(previous, ls[:, tail:])
            top = next_top - mm2(bottom, lnext[...])
            top = jnp.where(has_right, top, 0.0).astype(BF16)
            prev16 = previous.astype(BF16)
            halo_wait_send(it)

            def update(k):
                c = slice(k * band, (k + 1) * band)
                x[:, c] = x[:, c] + (loc[:, c] - dot(top, us[:, c]) - dot(prev16, ls[:, c]))

            update(0)
            update(blocks - 1)
            halo_start(it + 1)
            for k in range(1, blocks - 1):
                update(k)
            pl.when(has_left)(nt_copy.wait_send)
            for c in a_copies:
                c.wait_send()
            for c in p_copies:
                c.wait_send()
            if groups > 1:
                pl.when(g < groups - 1)(b_copy.wait_send)
            if it == 0:
                for c in l_copies:
                    c.wait_send()
                pl.when(has_right)(u_copy.wait_send)
                pl.when(has_left)(t_copy.wait_send)

        out_ref[...] = x[...]
        residual(ITERS)
        partial = jnp.sum(nstack[...].T, axis=0, keepdims=True)
        nrow[...] = partial
        nbuf[me] = partial

        def norm_copy(k):
            return rcopy(nrow, nbuf.at[me], n_send.at[0], n_recv.at[0], lax.rem(me + k, n))

        @pl.loop(0, (n - 1) // 2)
        def _(i):
            norm_copy(n // 2 + i).start()
            norm_copy(n // 2 - 1 - i).start()

        norm_copy(n - 1).start()
        halo_wait_send(ITERS)
        everyone = nbuf.at[pl.ds(0, n - 1)]
        everything = rcopy(everyone, everyone, n_send.at[0], n_recv.at[0], right)
        everything.wait_recv()
        total = jnp.sqrt(jnp.sum(nbuf[...], axis=0) / order)
        for i in range(ITERS + 1):
            norm_ref[i:i + 1, :] = total[:, i * rhs:(i + 1) * rhs]
        everything.wait_send()

    return kernel


def body(b, x, dg, lo, up, z, us, ls):
    n = lax.axis_size("rows")
    rhs, cols = b.shape
    band = dg.shape[1]
    blocks = cols // band
    rb = rhs // SUB
    dma = pltpu.SemaphoreType.DMA
    vm = pltpu.VMEM
    scratch = [
        vm((rhs, cols), F32), vm((rhs, cols), F32), vm((3, cols, band), F32),
        vm(z.shape, BF16), vm(us.shape, BF16), vm(ls.shape, BF16),
        vm((3, blocks, band, band), BF16), vm((3, blocks, band, band), BF16),
        vm((GROUP, band, band), BF16),
        vm((GROUP + 1, band, band), BF16), vm((GROUP + 1, band, band), BF16),
        vm((band, band), BF16), vm((band, band), BF16),
        vm((ITERS + 1, rhs, band), F32), vm((ITERS + 1, rhs, band), F32),
        vm((rhs, cols), F32), vm((ITERS, rhs, band), F32),
        vm((ITERS, rb, 2, SUB, band), F32), vm((ITERS, GROUP, 2, SUB, band), F32),
        vm((ITERS, GROUP, SUB, band), F32),
        vm((ITERS, SUB, band), F32), vm((ITERS, SUB, band), F32),
        vm((ITERS, rb, SUB, band), F32), vm((ITERS, rb, SUB, band), F32),
        vm((LANES, LANES), F32), vm((1, LANES), F32), vm((n, 1, LANES), F32),
        dma((9,)), dma((GROUP,)), dma((GROUP,)), dma((2,)), dma((2,)),
        dma((ITERS + 1, 2)), dma((ITERS + 1, 2)),
        dma((ITERS,)), dma((ITERS,)), dma((ITERS, GROUP)), dma((ITERS, GROUP)),
        dma((ITERS,)), dma((ITERS,)), dma((ITERS, rb)), dma((ITERS, rb)),
        dma((1,)), dma((1,)),
    ]
    return pl.pallas_call(
        make_kernel(n, rhs, cols, band),
        out_shape=(
            jax.ShapeDtypeStruct((rhs, cols), F32),
            jax.ShapeDtypeStruct((ITERS + 1, rhs), F32),
        ),
        in_specs=[pl.BlockSpec(memory_space=pl.ANY)] * 8,
        out_specs=(pl.BlockSpec(memory_space=pltpu.VMEM),) * 2,
        scratch_shapes=scratch,
        compiler_params=pltpu.CompilerParams(
            collective_id=0, has_side_effects=True, vmem_limit_bytes=67043328
        ),
    )(b, x, dg, lo, up, z, us, ls)


def solution(mesh):
    return jax.shard_map(
        body,
        mesh=mesh,
        in_specs=(
            P(None, "rows"),
            P(None, "rows"),
            P("rows", None),
            P("rows", None),
            P("rows", None),
            P("rows", None),
            P(None, "rows"),
            P(None, "rows"),
        ),
        out_specs=(P(None, "rows"), P()),
        check_vma=False,
    )
```
